32 devices in a mesh: pool: 4 (over y, core), ga: 8 (over z, x).
Axes of the slice: x: 2, y: 2, z: 4, core: 2. Of those that a mesh axis runs over, the one named last changes fastest.
Arguments:
- coefficients: bfloat16 [4, 256, 2, 256, 128], P('pool', 'ga'), may hold values from -6 to 6
- stick_count: int32 [4, 8], P('pool', 'ga'), may hold values from 28 to 32, as said below
- dest_device: int32 [4, 256], P('pool', 'ga'), may hold values from -1 to 7, as said below
- dest_slot: int32 [4, 256], P('pool', 'ga'), may hold values from -1 to 31, as said below
- source_stick: int32 [4, 256], P('pool', 'ga'), may hold values from -1 to 255, as said below
Outputs:
- margins: float32 [4, 2, 256, 256], P('pool', None, 'ga')
The draws below stay inside these ranges and needn't reach their ends.
Inputs may be any that keep to these rules, and one draw needn't show every extreme that they name: Every k-point has a device whose 32 slots are all live; a device's live sticks are its first stick_count slots. `dest_device`: -1 exactly for sticks that land nowhere (among them all sticks that are not live); no device sends more than 8 of its sticks to one device, and some pair of devices reaches 8 for every k-point. `dest_slot`: -1 where dest_device is -1; the slots named are live slots of the layout of k-point q-1, no slot named twice. `source_stick`: the exact inverse of dest_device and dest_slot: a slot names a stick exactly when that stick names the slot, else -1.
All inputs are finite; a program needn't handle non-finite values.
Results may differ from the reference program's by a relative error of at most 0.0003.
Values may be sent and summed in bfloat16 or wider, within the bound.
A program may use at most 64 MiB of HBM per device.

```python
import jax
import jax.numpy as jnp
from jax import lax

NB = 256
PW = 128
SLOTS = 32
KPTS = 4
STICKS = 256
CAP = 8
N_GA = 8


def stick_maps(key):
    base_key = jax.random.fold_in(key, 7101)
    subkeys = jax.random.split(base_key, 6)
    lowest = SLOTS - max(1, SLOTS // 8)
    counts = jax.random.randint(subkeys[0], (KPTS, N_GA), lowest, SLOTS + 1)
    shifts = jax.random.randint(subkeys[1], (KPTS,), 0, N_GA)
    offsets = jax.vmap(lambda sub: jax.random.permutation(sub, N_GA))(jax.random.split(subkeys[2], KPTS))
    dest_order = jax.vmap(lambda sub: jax.random.permutation(sub, SLOTS))(jax.random.split(subkeys[3], KPTS * N_GA)).reshape(KPTS, N_GA, SLOTS)
    source_order = jax.vmap(lambda sub: jax.random.permutation(sub, SLOTS))(jax.random.split(subkeys[4], KPTS * N_GA)).reshape(KPTS, N_GA, SLOTS)
    full_dest = jax.random.randint(subkeys[5], (KPTS,), 0, N_GA)
    kpoint_list = jnp.arange(KPTS)
    counts = counts.at[(kpoint_list - 1) % KPTS, full_dest].set(SLOTS)
    full_source = (full_dest + shifts + offsets[:, 0]) % N_GA
    counts = counts.at[kpoint_list, full_source].set(SLOTS)
    shape = (KPTS, N_GA, SLOTS)
    device_grid = jnp.broadcast_to(jnp.arange(N_GA)[None, :, None], shape)
    kpoint_grid = jnp.broadcast_to(kpoint_list[:, None, None], shape)
    block_of = jnp.arange(SLOTS) // CAP
    chosen = offsets[:, block_of][:, None, :]
    source_dev = (device_grid + shifts[:, None, None] + chosen) % N_GA
    source_slot = jnp.take_along_axis(source_order, source_dev, axis=1)
    prev_counts = jnp.roll(counts, 1, axis=0)
    dest_live = dest_order < prev_counts[:, :, None]
    source_counts = jnp.take_along_axis(counts, source_dev.reshape(KPTS, N_GA * SLOTS), axis=1).reshape(shape)
    source_live = source_slot < source_counts
    valid = dest_live & source_live
    empty = jnp.full(shape, -1, jnp.int32)
    source_stick = empty.at[kpoint_grid, device_grid, dest_order].set(jnp.where(valid, source_dev * SLOTS + source_slot, -1).astype(jnp.int32))
    dest_device = empty.at[kpoint_grid, source_dev, source_slot].set(jnp.where(valid, device_grid, -1).astype(jnp.int32))
    dest_slot = empty.at[kpoint_grid, source_dev, source_slot].set(jnp.where(valid, dest_order, -1).astype(jnp.int32))
    flat_shape = (KPTS, N_GA * SLOTS)
    return (counts.astype(jnp.int32), dest_device.reshape(flat_shape), dest_slot.reshape(flat_shape), source_stick.reshape(flat_shape))


def draw_stick_count(key, part):
    return stick_maps(key)[0]


def draw_dest_device(key, part):
    return stick_maps(key)[1]


def draw_dest_slot(key, part):
    return stick_maps(key)[2]


def draw_source_stick(key, part):
    return stick_maps(key)[3]


def block_scale(own_key, dims, cuts, low, top_value):
    def one(position, shards_of):
        heights = jax.random.uniform(jax.random.fold_in(jax.random.fold_in(own_key, 6), position), (shards_of,), jnp.float32, low / len(cuts), top_value / len(cuts))
        return jnp.repeat(jnp.exp(heights), dims[position] // shards_of).reshape((-1,) + (1,) * (len(dims) - position - 1))

    gain = one(*cuts[0])
    for cut in cuts[1:]:
        gain = gain * one(*cut)
    return gain


def noise(own_key, extent, width, bound, pieces=(), kind=jnp.bfloat16):
    array = jax.random.normal(own_key, extent, jnp.float32) * width
    if len(pieces) > 0:
        array = block_scale(own_key, extent, pieces, -0.22, 0.18) * array
    return jnp.clip(array, min=-bound, max=bound).astype(kind)


def setup_inputs(seed: int = 0) -> dict:
    streams_of = jax.random.split(jax.random.key(seed), 6)
    coefficients = noise(streams_of[0], (KPTS, STICKS, 2, NB, PW), 1.0, 6.0, ((0, 4), (1, 8)))
    stick_count = draw_stick_count(jax.random.fold_in(streams_of[5], 71), 0)
    dest_device = draw_dest_device(jax.random.fold_in(streams_of[5], 71), 0)
    dest_slot = draw_dest_slot(jax.random.fold_in(streams_of[5], 71), 0)
    source_stick = draw_source_stick(jax.random.fold_in(streams_of[5], 71), 0)
    return {"coefficients": coefficients, "stick_count": stick_count, "dest_device": dest_device, "dest_slot": dest_slot, "source_stick": source_stick}


def reference(coefficients, stick_count, dest_device, dest_slot, source_stick):
    norm_scale = jnp.float32((2 * STICKS * PW) ** -0.5)
    slot_index = (jnp.arange(STICKS) % SLOTS).astype(jnp.int32)
    owner_device = (jnp.arange(STICKS) // SLOTS).astype(jnp.int32)
    results = []
    for kpoint in range(KPTS):
        neighbour = (kpoint + 1) % KPTS
        live_mask = slot_index < stick_count[kpoint][owner_device]
        bra_rows = jnp.where(live_mask[:, None, None, None], coefficients[kpoint], 0).astype(jnp.float32)
        anchor = source_stick[neighbour]
        safe_index = jnp.clip(anchor, 0, STICKS - 1).astype(jnp.int32)
        agreeing = (anchor >= 0) & (dest_device[neighbour][safe_index] == owner_device) & (dest_slot[neighbour][safe_index] == slot_index)
        ket_rows = jnp.where(agreeing[:, None, None, None], coefficients[neighbour][safe_index], 0).astype(jnp.float32)
        swapped = jnp.stack([ket_rows[:, 1], -ket_rows[:, 0]], axis=1)
        real_part = jnp.einsum('scmg,scng->mn', bra_rows, ket_rows, precision=lax.Precision.HIGHEST)
        imag_part = jnp.einsum('scmg,scng->mn', bra_rows, swapped, precision=lax.Precision.HIGHEST)
        results.append(jnp.stack([real_part, imag_part]) * norm_scale)
    return jnp.stack(results)
```

```python
import jax
import jax.numpy as jnp
from jax import lax
from jax.sharding import PartitionSpec as P


def passed_along(value, axis, steps):
    count = lax.axis_size(axis)
    pairs = [(source, (source + steps) % count) for source in range(count)]
    return lax.ppermute(value, axis, pairs)


def local(coefficients, stick_count, dest_device, dest_slot, source_stick):
    groups = lax.axis_size("ga")
    slot_count = coefficients.shape[1]
    bands = coefficients.shape[3]
    plane_waves = coefficients.shape[4]
    width = plane_waves // groups
    sticks = groups * slot_count
    norm_scale = (2 * groups * slot_count * plane_waves) ** (-0.5)
    split = coefficients[0].reshape(slot_count, 2, bands, groups, width)
    split = split.transpose(3, 0, 1, 4, 2)
    mine = lax.all_to_all(split, "ga", split_axis=0, concat_axis=0, tiled=True)
    mine = mine.reshape(sticks, 2 * width * bands)
    theirs = passed_along(mine, "pool", -1)
    anchor = passed_along(source_stick[0], "pool", -1)
    slot_list = jnp.arange(slot_count, dtype=jnp.int32)
    anchor = jnp.where(slot_list < stick_count[0, 0], anchor, -1)
    anchors = lax.all_gather(anchor, "ga", tiled=True)
    placer = (anchors[:, None] == jnp.arange(sticks, dtype=jnp.int32)[None, :]).astype(jnp.bfloat16)
    ket = jnp.dot(placer, theirs, preferred_element_type=jnp.float32).astype(jnp.bfloat16)
    bra = mine.reshape(sticks, 2, width, bands)
    ket = ket.reshape(sticks, 2, width, bands)
    swapped = jnp.stack([ket[:, 1], -ket[:, 0]], axis=1)
    real_part = jnp.einsum("scgm,scgn->mn", bra, ket, preferred_element_type=jnp.float32)
    imag_part = jnp.einsum("scgm,scgn->mn", bra, swapped, preferred_element_type=jnp.float32)
    partial_value = jnp.stack([real_part, imag_part])
    owned = lax.psum_scatter(partial_value, "ga", scatter_dimension=1, tiled=True)
    return (owned * norm_scale)[None]


def solution(mesh):
    return jax.shard_map(
        local,
        mesh=mesh,
        in_specs=(
            P("pool", "ga", None, None, None),
            P("pool", "ga"),
            P("pool", "ga"),
            P("pool", "ga"),
            P("pool", "ga"),
        ),
        out_specs=P("pool", None, "ga", None),
        check_vma=False,
    )
```

```python
import functools

import jax
import jax.numpy as jnp
from jax import lax
from jax.experimental import pallas as pl
from jax.experimental.pallas import tpu as pltpu
from jax.sharding import PartitionSpec as P

MESH = pl.DeviceIdType.MESH
CHUNKS = 8


def kernel(
    scale, coef, count, source, out,
    stage, send, mine, theirs, ket, acc, rs, near_map, far_map, slot_map,
    load_sem, own_sem, send_sem, recv_sem, fsend_sem, frecv_sem,
    map_send, map_recv, fmap_send, fmap_recv, map_sem, rs_send, rs_recv,
):
    groups, pools = lax.axis_size("ga"), lax.axis_size("pool")
    me, pool = lax.axis_index("ga"), lax.axis_index("pool")
    prev, succ = lax.rem(pool + pools - 1, pools), lax.rem(pool + 1, pools)
    slots, _, bands, waves = stage.shape
    width = waves // groups
    depth = 2 * width
    part = slots // CHUNKS
    half = bands // 2
    rows = bands // groups

    def load(c):
        span = pl.ds(c * part, part)
        return pltpu.make_async_copy(coef.at[0, span], stage.at[span], load_sem.at[c])

    def own(c):
        return pltpu.make_async_copy(
            send.at[me, pl.ds(c * part, part)],
            mine.at[pl.ds(me * slots + c * part, part)],
            own_sem.at[c],
        )

    def exchange(c, r):
        dest = lax.rem(me + r, groups)
        return pltpu.make_async_remote_copy(
            src_ref=send.at[dest, pl.ds(c * part, part)],
            dst_ref=mine.at[pl.ds(me * slots + c * part, part)],
            send_sem=send_sem.at[c, r],
            recv_sem=recv_sem.at[c, r],
            device_id={"ga": dest},
            device_id_type=MESH,
        )

    def forward(c, r):
        origin = lax.rem(me + groups - r, groups)
        span = pl.ds(origin * slots + c * part, part)
        return pltpu.make_async_remote_copy(
            src_ref=mine.at[span],
            dst_ref=theirs.at[span],
            send_sem=fsend_sem.at[c, r],
            recv_sem=frecv_sem.at[c, r],
            device_id={"pool": prev},
            device_id_type=MESH,
        )

    def map_copy(r):
        dest = lax.rem(me + r, groups)
        return pltpu.make_async_remote_copy(
            src_ref=source,
            dst_ref=near_map.at[me],
            send_sem=map_send.at[r],
            recv_sem=map_recv.at[r],
            device_id={"ga": dest},
            device_id_type=MESH,
        )

    def map_forward():
        return pltpu.make_async_remote_copy(
            src_ref=near_map,
            dst_ref=far_map,
            send_sem=fmap_send,
            recv_sem=fmap_recv,
            device_id={"pool": prev},
            device_id_type=MESH,
        )

    for c in range(CHUNKS):
        load(c).start()
    own_map = pltpu.make_async_copy(source, near_map.at[me], map_sem)
    own_map.start()

    barrier = pltpu.get_barrier_semaphore()
    for r in range(1, groups):
        pl.semaphore_signal(
            barrier, inc=1, device_id={"ga": lax.rem(me + r, groups)}, device_id_type=MESH
        )
    for other in (prev, succ):
        pl.semaphore_signal(barrier, inc=1, device_id={"pool": other}, device_id_type=MESH)

    def transposed(c):
        load(c).wait()
        for s in range(part):
            slot = c * part + s
            live = slot < count[0, 0]
            for k in range(2):
                block = stage[slot, k]
                block = jnp.where(live, block, jnp.zeros_like(block)).T
                send[:, slot, k * width:(k + 1) * width, :] = block.reshape(groups, width, bands)

    order = [groups // 2] + [r for d in range(1, groups // 2) for r in (groups // 2 - d, groups // 2 + d)]
    order = order[: groups - 1]

    def send_chunk(c):
        for r in order:
            exchange(c, r).start()
        own(c).start()

    transposed(0)
    pl.semaphore_wait(barrier, groups + 1)

    def step(c, carry):
        transposed(c)
        send_chunk(c - 1)
        return carry

    lax.fori_loop(1, CHUNKS, step, 0)
    own_map.wait()
    for r in range(1, groups):
        map_copy(r).start()
    send_chunk(CHUNKS - 1)
    for r in range(1, groups):
        map_copy(r).wait()
    map_forward().start()

    def pass_on(c, carry):
        own(c).wait()
        forward(c, 0).start()
        for r in order[::-1]:
            exchange(c, r).wait_recv()
            forward(c, r).start()
        return carry

    lax.fori_loop(0, CHUNKS, pass_on, 0)
    map_forward().wait()
    to_scalar = pltpu.make_async_copy(far_map, slot_map, map_sem)
    to_scalar.start()
    to_scalar.wait()

    def arrived(c, carry):
        for r in range(groups):
            forward(c, r).wait_recv()
        return carry

    lax.fori_loop(0, CHUNKS, arrived, 0)

    near_half = me // (groups // 2)
    far_half = 1 - near_half

    def gather(b):
        for s in range(slots):
            index = slot_map[b, 0, s]
            block = theirs[jnp.maximum(index, 0)]
            block = jnp.where(index >= 0, block, jnp.zeros_like(block))
            span = pl.ds((b * slots + s) * depth, depth)
            ket[span, 0:bands] = block
            ket[span, bands:2 * bands] = jnp.concatenate([block[width:], -block[:width]], axis=0)

    def product(b, side):
        columns = pl.ds(pl.multiple_of(side * half, half), half)
        bra = mine[pl.ds(b * slots, slots), :, columns].reshape(slots * depth, half)
        other = ket[pl.ds(b * slots * depth, slots * depth), :]
        value = lax.dot_general(
            bra, other, (((0,), (0,)), ((), ())), preferred_element_type=jnp.float32
        )
        span = pl.ds(side * half, half)
        acc[span, :] += value

    acc[...] = jnp.zeros_like(acc)

    def far_step(b, carry):
        gather(b)
        product(b, far_half)
        return carry

    lax.fori_loop(0, groups, far_step, 0)

    def piece(dest):
        return pltpu.make_async_remote_copy(
            src_ref=acc.at[pl.ds(dest * rows, rows)],
            dst_ref=rs.at[me],
            send_sem=rs_send.at[dest],
            recv_sem=rs_recv.at[me],
            device_id={"ga": dest},
            device_id_type=MESH,
        )

    def landed(origin):
        return pltpu.make_async_remote_copy(
            src_ref=acc.at[pl.ds(origin * rows, rows)],
            dst_ref=rs.at[origin],
            send_sem=rs_send.at[origin],
            recv_sem=rs_recv.at[origin],
            device_id={"ga": origin},
            device_id_type=MESH,
        )

    product(0, near_half)
    mates = groups // 2
    for j in range(mates):
        piece(far_half * mates + lax.rem(me + j, mates)).start()

    def near_step(b, carry):
        product(b, near_half)
        return carry

    lax.fori_loop(1, groups, near_step, 0)
    total = acc[pl.ds(me * rows, rows), :]
    rs[pl.ds(me, 1)] = total[None]
    for j in range(1, mates):
        piece(near_half * mates + lax.rem(me + j, mates)).start()
    for r in range(1, groups):
        landed(lax.rem(me + r, groups)).wait_recv()
    total = rs[0]
    for g in range(1, groups):
        total = total + rs[g]
    total = total * scale
    out[0, 0] = total[:, :bands]
    out[0, 1] = total[:, bands:]

    def drain(c, carry):
        for r in range(groups):
            forward(c, r).wait_send()
        for r in range(1, groups):
            exchange(c, r).wait_send()
        return carry

    lax.fori_loop(0, CHUNKS, drain, 0)
    for r in range(1, groups):
        landed(lax.rem(me + r, groups)).wait_send()


def in_one_kernel(coefficients, stick_count, dest_device, dest_slot, source_stick):
    groups = lax.axis_size("ga")
    _, slots, _, bands, waves = coefficients.shape
    depth = 2 * waves // groups
    sticks = groups * slots
    rows = bands // groups
    scale = (2 * sticks * waves) ** (-0.5)
    any_space = pl.BlockSpec(memory_space=pl.ANY)
    sems = pltpu.SemaphoreType.DMA
    grid_sems = sems((CHUNKS, groups))
    return pl.pallas_call(
        functools.partial(kernel, scale),
        out_shape=jax.ShapeDtypeStruct((1, 2, rows, bands), jnp.float32),
        in_specs=[any_space, pl.BlockSpec(memory_space=pltpu.SMEM), pl.BlockSpec(memory_space=pltpu.VMEM)],
        out_specs=pl.BlockSpec(memory_space=pltpu.VMEM),
        scratch_shapes=[
            pltpu.VMEM((slots, 2, bands, waves), coefficients.dtype),
            pltpu.VMEM((groups, slots, depth, bands), coefficients.dtype),
            pltpu.VMEM((sticks, depth, bands), coefficients.dtype),
            pltpu.VMEM((sticks, depth, bands), coefficients.dtype),
            pltpu.VMEM((sticks * depth, 2 * bands), coefficients.dtype),
            pltpu.VMEM((bands, 2 * bands), jnp.float32),
            pltpu.VMEM((groups, rows, 2 * bands), jnp.float32),
            pltpu.VMEM((groups, 1, slots), jnp.int32),
            pltpu.VMEM((groups, 1, slots), jnp.int32),
            pltpu.SMEM((groups, 1, slots), jnp.int32),
            sems((CHUNKS,)), sems((CHUNKS,)),
            grid_sems, grid_sems, grid_sems, grid_sems,
            sems((groups,)), sems((groups,)), sems, sems, sems,
            sems((groups,)), sems((groups,)),
        ],
        compiler_params=pltpu.CompilerParams(collective_id=0, has_side_effects=True, vmem_limit_bytes=60 * 1024 * 1024),
    )(coefficients, stick_count, source_stick)


def passed_along(value, axis, steps):
    count = lax.axis_size(axis)
    pairs = [(source, (source + steps) % count) for source in range(count)]
    return lax.ppermute(value, axis, pairs)


def with_collectives(coefficients, stick_count, dest_device, dest_slot, source_stick):
    groups = lax.axis_size("ga")
    slot_count = coefficients.shape[1]
    bands = coefficients.shape[3]
    plane_waves = coefficients.shape[4]
    width = plane_waves // groups
    sticks = groups * slot_count
    norm_scale = (2 * groups * slot_count * plane_waves) ** (-0.5)
    split = coefficients[0].reshape(slot_count, 2, bands, groups, width)
    split = split.transpose(3, 0, 1, 4, 2)
    mine = lax.all_to_all(split, "ga", split_axis=0, concat_axis=0, tiled=True)
    mine = mine.reshape(sticks, 2 * width * bands)
    theirs = passed_along(mine, "pool", -1)
    anchor = passed_along(source_stick[0], "pool", -1)
    slot_list = jnp.arange(slot_count, dtype=jnp.int32)
    anchor = jnp.where(slot_list < stick_count[0, 0], anchor, -1)
    anchors = lax.all_gather(anchor, "ga", tiled=True)
    placer = (anchors[:, None] == jnp.arange(sticks, dtype=jnp.int32)[None, :]).astype(jnp.bfloat16)
    ket = jnp.dot(placer, theirs, preferred_element_type=jnp.float32).astype(jnp.bfloat16)
    bra = mine.reshape(sticks, 2, width, bands)
    ket = ket.reshape(sticks, 2, width, bands)
    swapped = jnp.stack([ket[:, 1], -ket[:, 0]], axis=1)
    real_part = jnp.einsum("scgm,scgn->mn", bra, ket, preferred_element_type=jnp.float32)
    imag_part = jnp.einsum("scgm,scgn->mn", bra, swapped, preferred_element_type=jnp.float32)
    partial_value = jnp.stack([real_part, imag_part])
    owned = lax.psum_scatter(partial_value, "ga", scatter_dimension=1, tiled=True)
    return (owned * norm_scale)[None]


def local(coefficients, *rest):
    width = coefficients.shape[4] // lax.axis_size("ga")
    if width % 16 == 0 and coefficients.shape[1] % CHUNKS == 0:
        return in_one_kernel(coefficients, *rest)
    return with_collectives(coefficients, *rest)


def solution(mesh):
    return jax.shard_map(
        local,
        mesh=mesh,
        in_specs=(
            P("pool", "ga", None, None, None),
            P("pool", "ga"),
            P("pool", "ga"),
            P("pool", "ga"),
            P("pool", "ga"),
        ),
        out_specs=P("pool", None, "ga", None),
        check_vma=False,
    )
```

```python
import functools

import jax
import jax.numpy as jnp
from jax import lax
from jax.experimental import pallas as pl
from jax.experimental.pallas import tpu as pltpu
from jax.sharding import PartitionSpec as P

MESH = pl.DeviceIdType.MESH
CHUNKS = 8
WINDOW = 2


def kernel(
    scale, coef, count, source, out,
    stage, send, mine, theirs, ket, acc, rs, near_map, far_map, slot_map,
    load_sem, own_sem, send_sem, recv_sem, fsend_sem, frecv_sem,
    map_send, map_recv, fmap_send, fmap_recv, map_sem, rs_send, rs_recv,
):
    groups, pools = lax.axis_size("ga"), lax.axis_size("pool")
    me, pool = lax.axis_index("ga"), lax.axis_index("pool")
    prev, succ = lax.rem(pool + pools - 1, pools), lax.rem(pool + 1, pools)
    slots, _, bands, waves = stage.shape
    width = waves // groups
    depth = 2 * width
    part = slots // CHUNKS
    half = bands // 2
    rows = bands // groups

    def load(c):
        span = pl.ds(c * part, part)
        return pltpu.make_async_copy(coef.at[0, span], stage.at[span], load_sem.at[c])

    def own(c):
        return pltpu.make_async_copy(
            send.at[me, pl.ds(c * part, part)],
            mine.at[pl.ds(me * slots + c * part, part)],
            own_sem.at[c],
        )

    def exchange(c, r):
        dest = lax.rem(me + r, groups)
        return pltpu.make_async_remote_copy(
            src_ref=send.at[dest, pl.ds(c * part, part)],
            dst_ref=mine.at[pl.ds(me * slots + c * part, part)],
            send_sem=send_sem.at[c, r],
            recv_sem=recv_sem.at[c, r],
            device_id={"ga": dest},
            device_id_type=MESH,
        )

    def forward(c, r):
        origin = lax.rem(me + groups - r, groups)
        span = pl.ds(origin * slots + c * part, part)
        return pltpu.make_async_remote_copy(
            src_ref=mine.at[span],
            dst_ref=theirs.at[span],
            send_sem=fsend_sem.at[c, r],
            recv_sem=frecv_sem.at[c, r],
            device_id={"pool": prev},
            device_id_type=MESH,
        )

    def map_copy(r):
        dest = lax.rem(me + r, groups)
        return pltpu.make_async_remote_copy(
            src_ref=source,
            dst_ref=near_map.at[me],
            send_sem=map_send.at[r],
            recv_sem=map_recv.at[r],
            device_id={"ga": dest},
            device_id_type=MESH,
        )

    def map_forward():
        return pltpu.make_async_remote_copy(
            src_ref=near_map,
            dst_ref=far_map,
            send_sem=fmap_send,
            recv_sem=fmap_recv,
            device_id={"pool": prev},
            device_id_type=MESH,
        )

    for c in range(CHUNKS):
        load(c).start()
    own_map = pltpu.make_async_copy(source, near_map.at[me], map_sem)
    own_map.start()

    barrier = pltpu.get_barrier_semaphore()
    for r in range(1, groups):
        pl.semaphore_signal(
            barrier, inc=1, device_id={"ga": lax.rem(me + r, groups)}, device_id_type=MESH
        )
    for other in (prev, succ):
        pl.semaphore_signal(barrier, inc=1, device_id={"pool": other}, device_id_type=MESH)

    def transposed(c):
        load(c).wait()
        for s in range(part):
            slot = c * part + s
            live = slot < count[0, 0]
            for k in range(2):
                block = stage[slot, k]
                block = jnp.where(live, block, jnp.zeros_like(block)).T
                send[:, slot, k * width:(k + 1) * width, :] = block.reshape(groups, width, bands)

    order = [groups // 2] + [r for d in range(1, groups // 2) for r in (groups // 2 - d, groups // 2 + d)]
    order = order[: groups - 1]

    def send_chunk(c):
        for r in order:
            exchange(c, r).start()
        own(c).start()

    def pass_on(c):
        own(c).wait()
        forward(c, 0).start()
        for r in order[::-1]:
            exchange(c, r).wait_recv()
            forward(c, r).start()

    def feed(c, carry):
        transposed(c)
        pass_on(c - WINDOW)
        send_chunk(c)
        return carry

    def finish(c, carry):
        pass_on(c)
        return carry

    transposed(0)
    pl.semaphore_wait(barrier, groups + 1)
    for c in range(1, WINDOW):
        transposed(c)
        send_chunk(c - 1)
    own_map.wait()
    for r in range(1, groups):
        map_copy(r).start()
    send_chunk(WINDOW - 1)
    lax.fori_loop(WINDOW, CHUNKS, feed, 0)
    for r in range(1, groups):
        map_copy(r).wait()
    map_forward().start()
    lax.fori_loop(CHUNKS - WINDOW, CHUNKS, finish, 0)
    map_forward().wait()
    to_scalar = pltpu.make_async_copy(far_map, slot_map, map_sem)
    to_scalar.start()
    to_scalar.wait()

    def arrived(c, carry):
        for r in range(groups):
            forward(c, r).wait_recv()
        return carry

    lax.fori_loop(0, CHUNKS, arrived, 0)

    near_half = me // (groups // 2)
    far_half = 1 - near_half

    def gather(b):
        for s in range(slots):
            index = slot_map[b, 0, s]
            block = theirs[jnp.maximum(index, 0)]
            block = jnp.where(index >= 0, block, jnp.zeros_like(block))
            span = pl.ds((b * slots + s) * depth, depth)
            ket[span, 0:bands] = block
            ket[span, bands:2 * bands] = jnp.concatenate([block[width:], -block[:width]], axis=0)

    def product(b, side):
        columns = pl.ds(pl.multiple_of(side * half, half), half)
        bra = mine[pl.ds(b * slots, slots), :, columns].reshape(slots * depth, half)
        other = ket[pl.ds(b * slots * depth, slots * depth), :]
        value = lax.dot_general(
            bra, other, (((0,), (0,)), ((), ())), preferred_element_type=jnp.float32
        )
        span = pl.ds(side * half, half)
        acc[span, :] += value

    acc[...] = jnp.zeros_like(acc)

    def far_step(b, carry):
        gather(b)
        product(b, far_half)
        return carry

    lax.fori_loop(0, groups, far_step, 0)

    def piece(dest):
        return pltpu.make_async_remote_copy(
            src_ref=acc.at[pl.ds(dest * rows, rows)],
            dst_ref=rs.at[me],
            send_sem=rs_send.at[dest],
            recv_sem=rs_recv.at[me],
            device_id={"ga": dest},
            device_id_type=MESH,
        )

    def landed(origin):
        return pltpu.make_async_remote_copy(
            src_ref=acc.at[pl.ds(origin * rows, rows)],
            dst_ref=rs.at[origin],
            send_sem=rs_send.at[origin],
            recv_sem=rs_recv.at[origin],
            device_id={"ga": origin},
            device_id_type=MESH,
        )

    product(0, near_half)
    mates = groups // 2
    for j in range(mates):
        piece(far_half * mates + lax.rem(me + j, mates)).start()

    def near_step(b, carry):
        product(b, near_half)
        return carry

    lax.fori_loop(1, groups, near_step, 0)
    total = acc[pl.ds(me * rows, rows), :]
    rs[pl.ds(me, 1)] = total[None]
    for j in range(1, mates):
        piece(near_half * mates + lax.rem(me + j, mates)).start()
    for r in range(1, groups):
        landed(lax.rem(me + r, groups)).wait_recv()
    total = rs[0]
    for g in range(1, groups):
        total = total + rs[g]
    total = total * scale
    out[0, 0] = total[:, :bands]
    out[0, 1] = total[:, bands:]

    def drain(c, carry):
        for r in range(groups):
            forward(c, r).wait_send()
        for r in range(1, groups):
            exchange(c, r).wait_send()
        return carry

    lax.fori_loop(0, CHUNKS, drain, 0)
    for r in range(1, groups):
        landed(lax.rem(me + r, groups)).wait_send()


def in_one_kernel(coefficients, stick_count, dest_device, dest_slot, source_stick):
    groups = lax.axis_size("ga")
    _, slots, _, bands, waves = coefficients.shape
    depth = 2 * waves // groups
    sticks = groups * slots
    rows = bands // groups
    scale = (2 * sticks * waves) ** (-0.5)
    any_space = pl.BlockSpec(memory_space=pl.ANY)
    sems = pltpu.SemaphoreType.DMA
    grid_sems = sems((CHUNKS, groups))
    return pl.pallas_call(
        functools.partial(kernel, scale),
        out_shape=jax.ShapeDtypeStruct((1, 2, rows, bands), jnp.float32),
        in_specs=[any_space, pl.BlockSpec(memory_space=pltpu.SMEM), pl.BlockSpec(memory_space=pltpu.VMEM)],
        out_specs=pl.BlockSpec(memory_space=pltpu.VMEM),
        scratch_shapes=[
            pltpu.VMEM((slots, 2, bands, waves), coefficients.dtype),
            pltpu.VMEM((groups, slots, depth, bands), coefficients.dtype),
            pltpu.VMEM((sticks, depth, bands), coefficients.dtype),
            pltpu.VMEM((sticks, depth, bands), coefficients.dtype),
            pltpu.VMEM((sticks * depth, 2 * bands), coefficients.dtype),
            pltpu.VMEM((bands, 2 * bands), jnp.float32),
            pltpu.VMEM((groups, rows, 2 * bands), jnp.float32),
            pltpu.VMEM((groups, 1, slots), jnp.int32),
            pltpu.VMEM((groups, 1, slots), jnp.int32),
            pltpu.SMEM((groups, 1, slots), jnp.int32),
            sems((CHUNKS,)), sems((CHUNKS,)),
            grid_sems, grid_sems, grid_sems, grid_sems,
            sems((groups,)), sems((groups,)), sems, sems, sems,
            sems((groups,)), sems((groups,)),
        ],
        compiler_params=pltpu.CompilerParams(collective_id=0, has_side_effects=True, vmem_limit_bytes=60 * 1024 * 1024),
    )(coefficients, stick_count, source_stick)


def passed_along(value, axis, steps):
    count = lax.axis_size(axis)
    pairs = [(source, (source + steps) % count) for source in range(count)]
    return lax.ppermute(value, axis, pairs)


def with_collectives(coefficients, stick_count, dest_device, dest_slot, source_stick):
    groups = lax.axis_size("ga")
    slot_count = coefficients.shape[1]
    bands = coefficients.shape[3]
    plane_waves = coefficients.shape[4]
    width = plane_waves // groups
    sticks = groups * slot_count
    norm_scale = (2 * groups * slot_count * plane_waves) ** (-0.5)
    split = coefficients[0].reshape(slot_count, 2, bands, groups, width)
    split = split.transpose(3, 0, 1, 4, 2)
    mine = lax.all_to_all(split, "ga", split_axis=0, concat_axis=0, tiled=True)
    mine = mine.reshape(sticks, 2 * width * bands)
    theirs = passed_along(mine, "pool", -1)
    anchor = passed_along(source_stick[0], "pool", -1)
    slot_list = jnp.arange(slot_count, dtype=jnp.int32)
    anchor = jnp.where(slot_list < stick_count[0, 0], anchor, -1)
    anchors = lax.all_gather(anchor, "ga", tiled=True)
    placer = (anchors[:, None] == jnp.arange(sticks, dtype=jnp.int32)[None, :]).astype(jnp.bfloat16)
    ket = jnp.dot(placer, theirs, preferred_element_type=jnp.float32).astype(jnp.bfloat16)
    bra = mine.reshape(sticks, 2, width, bands)
    ket = ket.reshape(sticks, 2, width, bands)
    swapped = jnp.stack([ket[:, 1], -ket[:, 0]], axis=1)
    real_part = jnp.einsum("scgm,scgn->mn", bra, ket, preferred_element_type=jnp.float32)
    imag_part = jnp.einsum("scgm,scgn->mn", bra, swapped, preferred_element_type=jnp.float32)
    partial_value = jnp.stack([real_part, imag_part])
    owned = lax.psum_scatter(partial_value, "ga", scatter_dimension=1, tiled=True)
    return (owned * norm_scale)[None]


def local(coefficients, *rest):
    width = coefficients.shape[4] // lax.axis_size("ga")
    if width % 16 == 0 and coefficients.shape[1] % CHUNKS == 0:
        return in_one_kernel(coefficients, *rest)
    return with_collectives(coefficients, *rest)


def solution(mesh):
    return jax.shard_map(
        local,
        mesh=mesh,
        in_specs=(
            P("pool", "ga", None, None, None),
            P("pool", "ga"),
            P("pool", "ga"),
            P("pool", "ga"),
            P("pool", "ga"),
        ),
        out_specs=P("pool", None, "ga", None),
        check_vma=False,
    )
```

```python
import functools

import jax
import jax.numpy as jnp
from jax import lax
from jax.experimental import pallas as pl
from jax.experimental.pallas import tpu as pltpu
from jax.sharding import PartitionSpec as P

MESH = pl.DeviceIdType.MESH
CHUNKS = 8
WINDOW = 2


def kernel(
    scale, coef, count, source, out,
    stage, send, mine, theirs, ket, acc, rs, near_map, far_map, slot_map,
    load_sem, own_sem, send_sem, recv_sem, fsend_sem, frecv_sem,
    map_send, map_recv, fmap_send, fmap_recv, map_sem, rs_send, rs_recv,
):
    groups, pools = lax.axis_size("ga"), lax.axis_size("pool")
    me, pool = lax.axis_index("ga"), lax.axis_index("pool")
    prev, succ = lax.rem(pool + pools - 1, pools), lax.rem(pool + 1, pools)
    slots, _, bands, waves = stage.shape
    width = waves // groups
    depth = 2 * width
    part = slots // CHUNKS
    half = bands // 2
    rows = bands // groups

    def load(c):
        span = pl.ds(c * part, part)
        return pltpu.make_async_copy(coef.at[0, span], stage.at[span], load_sem.at[c])

    def own(c):
        return pltpu.make_async_copy(
            send.at[me, pl.ds(c * part, part)],
            mine.at[pl.ds(me * slots + c * part, part)],
            own_sem.at[c],
        )

    def exchange(c, r):
        dest = lax.rem(me + r, groups)
        return pltpu.make_async_remote_copy(
            src_ref=send.at[dest, pl.ds(c * part, part)],
            dst_ref=mine.at[pl.ds(me * slots + c * part, part)],
            send_sem=send_sem.at[c, r],
            recv_sem=recv_sem.at[c, r],
            device_id={"ga": dest},
            device_id_type=MESH,
        )

    def forward(c, r):
        origin = lax.rem(me + groups - r, groups)
        span = pl.ds(origin * slots + c * part, part)
        return pltpu.make_async_remote_copy(
            src_ref=mine.at[span],
            dst_ref=theirs.at[span],
            send_sem=fsend_sem.at[c, r],
            recv_sem=frecv_sem.at[c, r],
            device_id={"pool": prev},
            device_id_type=MESH,
        )

    def map_copy(r):
        dest = lax.rem(me + r, groups)
        return pltpu.make_async_remote_copy(
            src_ref=source,
            dst_ref=near_map.at[me],
            send_sem=map_send.at[r],
            recv_sem=map_recv.at[r],
            device_id={"ga": dest},
            device_id_type=MESH,
        )

    def map_forward():
        return pltpu.make_async_remote_copy(
            src_ref=near_map,
            dst_ref=far_map,
            send_sem=fmap_send,
            recv_sem=fmap_recv,
            device_id={"pool": prev},
            device_id_type=MESH,
        )

    for c in range(CHUNKS):
        load(c).start()
    own_map = pltpu.make_async_copy(source, near_map.at[me], map_sem)
    own_map.start()

    barrier = pltpu.get_barrier_semaphore()
    for r in range(1, groups):
        pl.semaphore_signal(
            barrier, inc=1, device_id={"ga": lax.rem(me + r, groups)}, device_id_type=MESH
        )
    for other in (prev, succ):
        pl.semaphore_signal(barrier, inc=1, device_id={"pool": other}, device_id_type=MESH)

    def transposed(c):
        load(c).wait()
        for s in range(part):
            slot = c * part + s
            live = slot < count[0, 0]
            for k in range(2):
                block = stage[slot, k]
                block = jnp.where(live, block, jnp.zeros_like(block)).T
                send[:, slot, k * width:(k + 1) * width, :] = block.reshape(groups, width, bands)

    order = [groups // 2] + [r for d in range(1, groups // 2) for r in (groups // 2 - d, groups // 2 + d)]
    order = order[: groups - 1]

    def send_chunk(c):
        for r in order:
            exchange(c, r).start()
        own(c).start()

    def pass_on(c):
        own(c).wait()
        forward(c, 0).start()
        for r in order[::-1]:
            exchange(c, r).wait_recv()
            forward(c, r).start()

    def feed(c, carry):
        transposed(c)
        pass_on(c - WINDOW)
        send_chunk(c)
        return carry

    def finish(c, carry):
        pass_on(c)
        return carry

    transposed(0)
    pl.semaphore_wait(barrier, groups + 1)
    send_chunk(0)
    for c in range(1, WINDOW):
        transposed(c)
    own_map.wait()
    for r in range(1, groups):
        map_copy(r).start()
    for c in range(1, WINDOW):
        send_chunk(c)
    acc[...] = jnp.zeros_like(acc)
    lax.fori_loop(WINDOW, CHUNKS, feed, 0)
    for r in range(1, groups):
        map_copy(r).wait()
    map_forward().start()
    lax.fori_loop(CHUNKS - WINDOW, CHUNKS, finish, 0)
    map_forward().wait()
    to_scalar = pltpu.make_async_copy(far_map, slot_map, map_sem)
    to_scalar.start()
    to_scalar.wait()

    def arrived(c, carry):
        for r in range(groups):
            forward(c, r).wait_recv()
        return carry

    lax.fori_loop(0, CHUNKS, arrived, 0)

    near_half = me // (groups // 2)
    far_half = 1 - near_half

    def gather(b):
        for s in range(slots):
            index = slot_map[b, 0, s]
            block = theirs[jnp.maximum(index, 0)]
            block = jnp.where(index >= 0, block, jnp.zeros_like(block))
            span = pl.ds((b * slots + s) * depth, depth)
            ket[span, 0:bands] = block
            ket[span, bands:2 * bands] = jnp.concatenate([block[width:], -block[:width]], axis=0)

    def product(b, side):
        columns = pl.ds(pl.multiple_of(side * half, half), half)
        bra = mine[pl.ds(b * slots, slots), :, columns].reshape(slots * depth, half)
        other = ket[pl.ds(b * slots * depth, slots * depth), :]
        value = lax.dot_general(
            bra, other, (((0,), (0,)), ((), ())), preferred_element_type=jnp.float32
        )
        span = pl.ds(side * half, half)
        acc[span, :] += value

    def far_step(b, carry):
        gather(b)
        product(b, far_half)
        return carry

    lax.fori_loop(0, groups, far_step, 0)

    def piece(dest):
        return pltpu.make_async_remote_copy(
            src_ref=acc.at[pl.ds(dest * rows, rows)],
            dst_ref=rs.at[me],
            send_sem=rs_send.at[dest],
            recv_sem=rs_recv.at[me],
            device_id={"ga": dest},
            device_id_type=MESH,
        )

    def landed(origin):
        return pltpu.make_async_remote_copy(
            src_ref=acc.at[pl.ds(origin * rows, rows)],
            dst_ref=rs.at[origin],
            send_sem=rs_send.at[origin],
            recv_sem=rs_recv.at[origin],
            device_id={"ga": origin},
            device_id_type=MESH,
        )

    product(0, near_half)
    mates = groups // 2
    for j in range(mates):
        piece(far_half * mates + lax.rem(me + j, mates)).start()

    def near_step(b, carry):
        product(b, near_half)
        return carry

    lax.fori_loop(1, groups, near_step, 0)
    total = acc[pl.ds(me * rows, rows), :]
    rs[pl.ds(me, 1)] = total[None]
    for j in range(1, mates):
        piece(near_half * mates + lax.rem(me + j, mates)).start()
    for r in range(1, groups):
        landed(lax.rem(me + r, groups)).wait_recv()
    total = rs[0]
    for g in range(1, groups):
        total = total + rs[g]
    total = total * scale
    out[0, 0] = total[:, :bands]
    out[0, 1] = total[:, bands:]

    def drain(c, carry):
        for r in range(groups):
            forward(c, r).wait_send()
        for r in range(1, groups):
            exchange(c, r).wait_send()
        return carry

    lax.fori_loop(0, CHUNKS, drain, 0)
    for r in range(1, groups):
        landed(lax.rem(me + r, groups)).wait_send()


def in_one_kernel(coefficients, stick_count, dest_device, dest_slot, source_stick):
    groups = lax.axis_size("ga")
    _, slots, _, bands, waves = coefficients.shape
    depth = 2 * waves // groups
    sticks = groups * slots
    rows = bands // groups
    scale = (2 * sticks * waves) ** (-0.5)
    any_space = pl.BlockSpec(memory_space=pl.ANY)
    sems = pltpu.SemaphoreType.DMA
    grid_sems = sems((CHUNKS, groups))
    return pl.pallas_call(
        functools.partial(kernel, scale),
        out_shape=jax.ShapeDtypeStruct((1, 2, rows, bands), jnp.float32),
        in_specs=[any_space, pl.BlockSpec(memory_space=pltpu.SMEM), pl.BlockSpec(memory_space=pltpu.VMEM)],
        out_specs=pl.BlockSpec(memory_space=pltpu.VMEM),
        scratch_shapes=[
            pltpu.VMEM((slots, 2, bands, waves), coefficients.dtype),
            pltpu.VMEM((groups, slots, depth, bands), coefficients.dtype),
            pltpu.VMEM((sticks, depth, bands), coefficients.dtype),
            pltpu.VMEM((sticks, depth, bands), coefficients.dtype),
            pltpu.VMEM((sticks * depth, 2 * bands), coefficients.dtype),
            pltpu.VMEM((bands, 2 * bands), jnp.float32),
            pltpu.VMEM((groups, rows, 2 * bands), jnp.float32),
            pltpu.VMEM((groups, 1, slots), jnp.int32),
            pltpu.VMEM((groups, 1, slots), jnp.int32),
            pltpu.SMEM((groups, 1, slots), jnp.int32),
            sems((CHUNKS,)), sems((CHUNKS,)),
            grid_sems, grid_sems, grid_sems, grid_sems,
            sems((groups,)), sems((groups,)), sems, sems, sems,
            sems((groups,)), sems((groups,)),
        ],
        compiler_params=pltpu.CompilerParams(collective_id=0, has_side_effects=True, vmem_limit_bytes=60 * 1024 * 1024),
    )(coefficients, stick_count, source_stick)


def passed_along(value, axis, steps):
    count = lax.axis_size(axis)
    pairs = [(source, (source + steps) % count) for source in range(count)]
    return lax.ppermute(value, axis, pairs)


def with_collectives(coefficients, stick_count, dest_device, dest_slot, source_stick):
    groups = lax.axis_size("ga")
    slot_count = coefficients.shape[1]
    bands = coefficients.shape[3]
    plane_waves = coefficients.shape[4]
    width = plane_waves // groups
    sticks = groups * slot_count
    norm_scale = (2 * groups * slot_count * plane_waves) ** (-0.5)
    split = coefficients[0].reshape(slot_count, 2, bands, groups, width)
    split = split.transpose(3, 0, 1, 4, 2)
    mine = lax.all_to_all(split, "ga", split_axis=0, concat_axis=0, tiled=True)
    mine = mine.reshape(sticks, 2 * width * bands)
    theirs = passed_along(mine, "pool", -1)
    anchor = passed_along(source_stick[0], "pool", -1)
    slot_list = jnp.arange(slot_count, dtype=jnp.int32)
    anchor = jnp.where(slot_list < stick_count[0, 0], anchor, -1)
    anchors = lax.all_gather(anchor, "ga", tiled=True)
    placer = (anchors[:, None] == jnp.arange(sticks, dtype=jnp.int32)[None, :]).astype(jnp.bfloat16)
    ket = jnp.dot(placer, theirs, preferred_element_type=jnp.float32).astype(jnp.bfloat16)
    bra = mine.reshape(sticks, 2, width, bands)
    ket = ket.reshape(sticks, 2, width, bands)
    swapped = jnp.stack([ket[:, 1], -ket[:, 0]], axis=1)
    real_part = jnp.einsum("scgm,scgn->mn", bra, ket, preferred_element_type=jnp.float32)
    imag_part = jnp.einsum("scgm,scgn->mn", bra, swapped, preferred_element_type=jnp.float32)
    partial_value = jnp.stack([real_part, imag_part])
    owned = lax.psum_scatter(partial_value, "ga", scatter_dimension=1, tiled=True)
    return (owned * norm_scale)[None]


def local(coefficients, *rest):
    width = coefficients.shape[4] // lax.axis_size("ga")
    if width % 16 == 0 and coefficients.shape[1] % CHUNKS == 0:
        return in_one_kernel(coefficients, *rest)
    return with_collectives(coefficients, *rest)


def solution(mesh):
    return jax.shard_map(
        local,
        mesh=mesh,
        in_specs=(
            P("pool", "ga", None, None, None),
            P("pool", "ga"),
            P("pool", "ga"),
            P("pool", "ga"),
            P("pool", "ga"),
        ),
        out_specs=P("pool", None, "ga", None),
        check_vma=False,
    )
```
